32 devices in a mesh: gx: 8 (over z, x), yz: 4 (over y, core).
Axes of the slice: x: 2, y: 2, z: 4, core: 2. Of those that a mesh axis runs over, the one named last changes fastest.
Arguments:
- populations: float32 [19, 64, 32, 128], P(None, 'gx', 'yz'), may hold values from 0.01 to 0.2
- solid: int32 [64, 32, 128], P('gx', 'yz'), may hold values 0 or 1
- displacement: float32 [3, 34816], P(None, ('gx', 'yz')), may hold values from -3 to 3
- stiffness: float32 [34816], P(('gx', 'yz')), may hold values from 0.05 to 0.5
- marker_tile: int32 [34816, 1], P(('gx', 'yz')), may hold values from 0 to 7, as said below
- marker_site: int32 [34816], P(('gx', 'yz')), may hold values from 0 to 8191
Outputs:
- final_populations: float32 [19, 64, 32, 128], P(None, 'gx', 'yz')
- final_displacement: float32 [3, 34816], P(None, ('gx', 'yz'))
The draws below stay inside these ranges and needn't reach their ends.
Inputs may be any that keep to these rules, and one draw needn't show every extreme that they name: `marker_tile`: among the rows of one device no value is named by more than 272 markers, and in every device's rows some value is named by exactly 272.
All inputs are finite; a program needn't handle non-finite values. No bound on the sum of `solid` on one device may be relied on, other than what follows from the above.
Results may differ from the reference program's by a relative error of at most 0.0003.
Values sent between devices are 32-bit elements; how exact they have to be, the bound alone decides.
No kernel may reach another device: no remote copies, remote signals or barrier semaphores. Data moves between devices by JAX's collectives and lax.ppermute only.
A program may use at most 128 MiB of HBM per device.

```python
import math
import jax
import jax.numpy as jnp

CX = 8
CY = 8
CZ = 128
STEPS = 3
TILE_SLOTS = 8
MARK_DEV = 1088
MARKERS = 34816
SITES_DEV = 8192
CAP = 272
NX = 64
NY = 32
NZ = 128
N_GX = 8
N_YZ = 4


def device_tiles(device_key):
    pick_key, slot_key, order_key = jax.random.split(device_key, 3)
    fullest = jax.random.randint(pick_key, (), 0, TILE_SLOTS).astype(jnp.int32)
    chosen = jax.random.permutation(slot_key, (TILE_SLOTS - 1) * CAP)[:MARK_DEV - CAP].astype(jnp.int32)
    others = (fullest + 1 + chosen // CAP) % TILE_SLOTS
    filled = jnp.zeros((CAP,), jnp.int32) + fullest
    values = jnp.concatenate([filled, others.astype(jnp.int32)], axis=0)
    order = jax.random.permutation(order_key, MARK_DEV).astype(jnp.int32)
    return values[order]


def draw_marker_tile(key, part):
    devices_count = MARKERS // MARK_DEV
    device_keys = jax.random.split(jax.random.fold_in(key, 71), devices_count)
    values = jax.vmap(device_tiles)(device_keys)
    return values.reshape(-1, 1).astype(jnp.int32)


def set_ends(entries, key, smallest, high):
    extent = entries.shape
    index_at = [jax.random.randint(jax.random.fold_in(key, axis), (), 0, extent[axis]) for axis in range(len(extent))]
    entries = entries.at[tuple(index_at)].set(smallest)
    longest = extent.index(max(extent))
    index_at[longest] = (index_at[longest] + 1) % extent[longest]
    return entries.at[tuple(index_at)].set(high)


def level_of(stream_key, shape, cuts, smallest, largest):
    def one(dim, shards_of):
        draws = jax.random.uniform(jax.random.fold_in(jax.random.fold_in(stream_key, 6), dim), (shards_of,), jnp.float32, smallest / len(cuts), largest / len(cuts))
        return jnp.repeat(jnp.exp(draws), shape[dim] // shards_of).reshape((-1,) + (1,) * (len(shape) - dim - 1))

    factor_of = one(*cuts[0])
    for cut in cuts[1:]:
        factor_of = factor_of * one(*cut)
    return factor_of


def scatter_about(key, dims, scale, most, cuts=(), held_as=jnp.bfloat16):
    values = jax.random.normal(key, dims, jnp.float32) * scale
    if len(cuts) > 0:
        values = level_of(key, dims, cuts, -0.22, 0.18) * values
    return jnp.clip(values, min=-most, max=most).astype(held_as)


def setup_inputs(seed: int = 0) -> dict:
    key_list = jax.random.split(jax.random.key(seed), 7)
    populations = jnp.clip(0.01 + 0.19 * jax.random.uniform(key_list[0], (19, NX, NY, NZ), jnp.float32) ** level_of(key_list[0], (19, NX, NY, NZ), ((1, 8), (2, 4)), -0.2, 0.2), 0.01, 0.2)
    solid = set_ends((jax.random.randint(key_list[1], (NX, NY, NZ), 0, 8) < 1).astype(jnp.int32), jax.random.fold_in(key_list[1], 1), 0, 1)
    displacement = scatter_about(key_list[2], (3, MARKERS), 0.5, 3.0, ((1, 32),), jnp.float32)
    stiffness = jnp.clip(jnp.exp(math.log(0.5) - 2.3025851 * jax.random.uniform(key_list[3], (MARKERS,), jnp.float32) ** level_of(key_list[3], (MARKERS,), ((0, 32),), -0.2, 0.2)), 0.05, 0.5)
    marker_tile = draw_marker_tile(jax.random.fold_in(key_list[6], 71), 0)
    marker_site = set_ends(jax.random.randint(key_list[5], (MARKERS,), 0, SITES_DEV), jax.random.fold_in(key_list[5], 1), 0, SITES_DEV - 1).astype(jnp.int32)
    return {"populations": populations, "solid": solid, "displacement": displacement, "stiffness": stiffness, "marker_tile": marker_tile, "marker_site": marker_site}


lattice_dirs = [(0, 0, 0), (1, 0, 0), (-1, 0, 0), (0, 1, 0), (0, -1, 0), (0, 0, 1), (0, 0, -1),
                (1, 1, 0), (-1, -1, 0), (1, -1, 0), (-1, 1, 0),
                (1, 0, 1), (-1, 0, -1), (1, 0, -1), (-1, 0, 1),
                (0, 1, 1), (0, -1, -1), (0, 1, -1), (0, -1, 1)]
lattice_weights = [1.0 / 3.0] + [1.0 / 18.0] * 6 + [1.0 / 36.0] * 12
opposite_dirs = [0, 2, 1, 4, 3, 6, 5, 8, 7, 10, 9, 12, 11, 14, 13, 16, 15, 18, 17]
relax_rate = 1.6


def weighted(offsets, parts, blank):
    total = blank
    for component in range(3):
        if offsets[component] != 0:
            total = total + offsets[component] * parts[component]
    return total


def collide(popul, field, solid):
    density = jnp.sum(popul, axis=0)
    moments = []
    for component in range(3):
        total = 0.5 * field[component]
        for index in range(19):
            offset = lattice_dirs[index][component]
            if offset != 0:
                total = total + offset * popul[index]
        moments.append(total / density)
    squared = moments[0] * moments[0] + moments[1] * moments[1] + moments[2] * moments[2]
    speed_field = moments[0] * field[0] + moments[1] * field[1] + moments[2] * field[2]
    blank = jnp.zeros_like(density)
    result = []
    for index in range(19):
        offsets = lattice_dirs[index]
        weight = lattice_weights[index]
        along = weighted(offsets, moments, blank)
        pushed = weighted(offsets, field, blank)
        drift = pushed - speed_field
        equil = weight * density * (1.0 + 3.0 * along + 4.5 * along * along - 1.5 * squared)
        source = (1.0 - 0.5 * relax_rate) * weight * (3.0 * drift + 9.0 * along * pushed)
        post = popul[index] - relax_rate * (popul[index] - equil) + source
        result.append(jnp.where(solid == 1, popul[opposite_dirs[index]], post))
    return jnp.stack(result), jnp.stack(moments)


def reference(populations, solid, displacement, stiffness, marker_tile, marker_site):
    total_rows = displacement.shape[1]
    rows = jnp.arange(total_rows, dtype=jnp.int32)
    owner = rows // MARK_DEV
    owner_x = owner // N_YZ
    value = marker_tile[:, 0]
    tile_x = (owner_x + value // N_YZ) % N_GX
    tile_y = value % N_YZ
    xs = tile_x * CX + marker_site // (CY * CZ)
    ys = tile_y * CY + (marker_site // CZ) % CY
    zs = marker_site % CZ
    flat = ((xs * NY + ys) * NZ + zs).astype(jnp.int32)
    popul = populations
    moved = displacement
    for step in range(STEPS):
        force = -stiffness[None, :] * moved
        field = jnp.zeros((3, NX * NY * NZ), jnp.float32).at[:, flat].add(force)
        field = field.reshape(3, NX, NY, NZ)
        post, speed = collide(popul, field, solid)
        moved = moved + speed.reshape(3, -1)[:, flat]
        popul = jnp.stack([jnp.roll(post[index], lattice_dirs[index], axis=(0, 1, 2)) for index in range(19)])
    return popul, moved
```

```python
import functools

import jax
import jax.numpy as jnp
from jax import lax
from jax.experimental import pallas as pl
from jax.experimental.pallas import tpu as pltpu
from jax.sharding import PartitionSpec as P

STEPS = 3

lattice_dirs = [
    (0, 0, 0),
    (1, 0, 0),
    (-1, 0, 0),
    (0, 1, 0),
    (0, -1, 0),
    (0, 0, 1),
    (0, 0, -1),
    (1, 1, 0),
    (-1, -1, 0),
    (1, -1, 0),
    (-1, 1, 0),
    (1, 0, 1),
    (-1, 0, -1),
    (1, 0, -1),
    (-1, 0, 1),
    (0, 1, 1),
    (0, -1, -1),
    (0, 1, -1),
    (0, -1, 1),
]
lattice_weights = [1.0 / 3.0] + [1.0 / 18.0] * 6 + [1.0 / 36.0] * 12
opposite_dirs = [0, 2, 1, 4, 3, 6, 5, 8, 7, 10, 9, 12, 11, 14, 13, 16, 15, 18, 17]
relax_rate = 1.6
Q19 = len(lattice_dirs)


f32 = jnp.float32
bf16 = jnp.bfloat16


def in_vmem(value):
    return pltpu.with_memory_space_constraint(value, pltpu.VMEM)


def call(kernel, args, outs, scratch=(), name=None, flops=0, hbm_outs=False):
    if hbm_outs:
        out_shape = [jax.ShapeDtypeStruct(shape, dtype) for shape, dtype in outs]
    else:
        out_shape = [pltpu.VMEM(shape, dtype) for shape, dtype in outs]
    spec = pl.BlockSpec(memory_space=pltpu.VMEM)
    return pl.pallas_call(
        kernel,
        out_shape=out_shape,
        in_specs=[spec] * len(args),
        out_specs=[spec] * len(outs),
        scratch_shapes=list(scratch),
        name=name,
        cost_estimate=pl.CostEstimate(flops=flops, transcendentals=0, bytes_accessed=0),
    )(*[in_vmem(arg) for arg in args])


def shifted(value, axis, steps):
    count = lax.axis_size(axis)
    pairs = [(source, (source + steps) % count) for source in range(count)]
    return lax.ppermute(value, axis, pairs)


def total_of(values):
    values = list(values)
    while len(values) > 1:
        paired = [values[i] + values[i + 1] for i in range(0, len(values) - 1, 2)]
        if len(values) % 2:
            paired.append(values[-1])
        values = paired
    return values[0]


def along(offsets, parts):
    total = None
    for component in range(3):
        if offsets[component] == 0:
            continue
        part = parts[component]
        if total is None:
            total = part if offsets[component] > 0 else -part
        else:
            total = total + part if offsets[component] > 0 else total - part
    return total


def collide(popul, field, solid):
    density = total_of(popul)
    inverse = 1.0 / density
    speed = []
    for component in range(3):
        plus = [popul[i] for i in range(Q19) if lattice_dirs[i][component] > 0]
        minus = [popul[i] for i in range(Q19) if lattice_dirs[i][component] < 0]
        total = total_of(plus) - total_of(minus) + 0.5 * field[component]
        speed.append(total * inverse)
    squared = total_of([part * part for part in speed])
    work = total_of([speed[c] * field[c] for c in range(3)])
    keep = 1.0 - relax_rate
    gain = 1.0 - 0.5 * relax_rate
    scaled = relax_rate * density
    base = scaled * (1.0 - 1.5 * squared) - (3.0 * gain) * work
    quad = 4.5 * scaled
    lin = 3.0 * scaled
    result = [None] * Q19
    for index in range(Q19):
        other = opposite_dirs[index]
        weight = lattice_weights[index]
        if index == other:
            post = keep * popul[index] + weight * base
            result[index] = jnp.where(solid, popul[index], post)
            continue
        if other < index:
            continue
        moved = along(lattice_dirs[index], speed)
        pushed = along(lattice_dirs[index], field)
        even = base + moved * (quad * moved + (9.0 * gain) * pushed)
        odd = lin * moved + (3.0 * gain) * pushed
        first = keep * popul[index] + weight * (even + odd)
        second = keep * popul[other] + weight * (even - odd)
        result[index] = jnp.where(solid, popul[other], first)
        result[other] = jnp.where(solid, popul[index], second)
    return result, speed


def rolled(value, index):
    steps = lattice_dirs[index][2]
    if steps == 0:
        return value
    size = value.shape[-1]
    return pltpu.roll(value, steps % size, len(value.shape) - 1)


def halo_entries(axis, sign, reach, extras):
    entries = []
    for layer in range(1, reach + 2):
        for index in range(Q19):
            if sign * lattice_dirs[index][axis] >= layer - reach:
                entries.append((index, layer))
    entries += [(Q19 + extra, 1) for extra in range(extras)]
    return entries


def corner_entries(sign_x, sign_y, reach, extras):
    rows = []
    for place, (index, layer_y) in enumerate(halo_entries(1, sign_y, reach, extras)):
        for layer_x in range(1, reach + 2):
            if index >= Q19:
                if layer_x == 1:
                    rows.append((place, layer_x, index, layer_y))
            elif sign_x * lattice_dirs[index][0] >= layer_x - reach:
                rows.append((place, layer_x, index, layer_y))
    return rows


def face_index(size, sign, layer):
    return size - layer if sign > 0 else layer - 1


def halo_index(size, sign, layer):
    return -layer if sign > 0 else size - 1 + layer


def round_up(count, unit):
    return (count + unit - 1) // unit * unit


def corner_kernel(reach, extras, nx, from_down, from_up, to_up, to_down):
    for sign_x, target in ((1, to_up), (-1, to_down)):
        at = 0
        for sign_y, source in ((1, from_down), (-1, from_up)):
            for place, layer_x, _, _ in corner_entries(sign_x, sign_y, reach, extras):
                column = face_index(nx, sign_x, layer_x)
                target[at : at + 1, :] = source[place, column : column + 1, :]
                at += 1
        if at < target.shape[0]:
            target[at:, :] = jnp.zeros((target.shape[0] - at, target.shape[1]), f32)


def corner_rows(reach, extras):
    return round_up(
        max(sum(len(corner_entries(x, y, reach, extras)) for y in (1, -1)) for x in (1, -1)), 8
    )


def fill_halo(buffer_of, pad, reach, extras, nx, ny, y_msgs, x_msgs, corners):
    for sign, message in ((1, y_msgs[0]), (-1, y_msgs[1])):
        for place, (index, layer) in enumerate(halo_entries(1, sign, reach, extras)):
            ref, at, margin = buffer_of(index)
            row = halo_index(ny, sign, layer) + margin
            ref[at, margin : margin + nx, row, :] = message[place]
    for sign, message in ((1, x_msgs[0]), (-1, x_msgs[1])):
        for place, (index, layer) in enumerate(halo_entries(0, sign, reach, extras)):
            ref, at, margin = buffer_of(index)
            ref[at, halo_index(nx, sign, layer) + margin, margin : margin + ny, :] = message[place]
    for sign_x, message in ((1, corners[0]), (-1, corners[1])):
        place = 0
        for sign_y in (1, -1):
            for _, layer_x, index, layer_y in corner_entries(sign_x, sign_y, reach, extras):
                ref, at, margin = buffer_of(index)
                column = halo_index(nx, sign_x, layer_x) + margin
                row = halo_index(ny, sign_y, layer_y) + margin
                ref[at, column, row : row + 1, :] = message[place : place + 1, :]
                place += 1


def send_faces(value_y, value_x, reach, extras, nx, ny, y_up, y_down, x_up, x_down):
    for sign, message in ((1, y_up), (-1, y_down)):
        for place, (index, layer) in enumerate(halo_entries(1, sign, reach, extras)):
            message[place] = value_y(index, face_index(ny, sign, layer))
    for sign, message in ((1, x_up), (-1, x_down)):
        for place, (index, layer) in enumerate(halo_entries(0, sign, reach, extras)):
            message[place] = value_x(index, face_index(nx, sign, layer))


def pack_kernel(nx, ny, nz, moved, stiff, tile, site, out):
    count = moved.shape[1]
    half = (nx // 2) * ny * nz
    place = site[...]
    high = place // half
    rest = place - high * half
    row = rest // nz
    lane = rest - row * nz + high * nz
    out[...] = jnp.concatenate(
        [jnp.zeros((6, out.shape[1]), f32), jnp.full((2, out.shape[1]), -1.0, f32)], axis=0
    )
    out[0:3, 0:count] = -stiff[...] * moved[...]
    out[3:4, 0:count] = stiff[...]
    out[4:5, 0:count] = lane.astype(f32)
    out[5:6, 0:count] = row.astype(f32)
    out[6:7, 0:count] = tile[...].astype(f32)


def one_hot(values, size, dtype=bf16):
    places = lax.broadcasted_iota(jnp.int32, (size, values.shape[1]), 0).astype(f32)
    return jnp.where(places == values, 1.0, 0.0).astype(dtype)


def two_parts(value):
    high = value.astype(bf16)
    low = (value - high.astype(f32)).astype(bf16)
    return high, low


def wanted_slot(far):
    slot = lax.axis_index("yz")
    if far:
        slot = slot + lax.axis_size("yz")
    return slot.astype(f32)


def marker_rows(raw, far):
    return jnp.where(raw[6:7, :] == wanted_slot(far), raw[5:6, :], -1.0)


def scatter_kernel(rows, lanes, far, count, *refs):
    out = refs[count]
    total = jnp.zeros((8 * rows, lanes), f32)
    for raw in refs[:count]:
        high, low = two_parts(raw[0:4, :])
        mask = one_hot(marker_rows(raw, far), rows)
        left = jnp.concatenate(
            [mask * part[c : c + 1, :] for part in (high, low) for c in range(4)], axis=0
        )
        right = one_hot(raw[4:5, :], lanes)
        total = total + lax.dot_general(
            left, right, (((1,), (1,)), ((), ())), preferred_element_type=f32
        )
    out[...] = total[: 4 * rows] + total[4 * rows :]


def gather_kernel(rows, lanes, count, speed, *refs):
    near, far, outs = refs[:count], refs[count : 2 * count], refs[2 * count :]
    high, low = two_parts(speed[...])
    table = jnp.concatenate([high, low], axis=0)
    for source in range(count):
        for kind, raw in enumerate((near[source], far[source])):
            right = one_hot(raw[4:5, :], lanes)
            picked = lax.dot_general(
                table, right, (((1,), (0,)), ((), ())), preferred_element_type=f32
            )
            mask = one_hot(marker_rows(raw, kind == 1), rows, f32)
            for c in range(3):
                part = (
                    picked[c * rows : (c + 1) * rows] + picked[(3 + c) * rows : (4 + c) * rows]
                )
                outs[source][3 * kind + c : 3 * kind + c + 1, :] = jnp.sum(
                    part * mask, axis=0, keepdims=True
                )
        outs[source][6:8, :] = jnp.zeros((2, outs[source].shape[1]), f32)


def own_sum_kernel(count, moved, *refs):
    parts, near_sum, far_sum = refs[:count], refs[count], refs[count + 1]
    number = moved.shape[1]
    total = total_of([part[...] for part in parts])
    near_sum[...] = moved[...] + total[0:3, 0:number]
    far_sum[0:3, :] = total[3:6, :]
    far_sum[3:8, :] = jnp.zeros((5, far_sum.shape[1]), f32)


def add_far_kernel(near_sum, far, out):
    out[...] = near_sum[...] + far[0:3, 0 : out.shape[1]]


def first_kernel(nx, ny, nz, popul, solid, near, far, post, field, slope, moved, *msgs):
    rows = (nx // 2) * ny
    for x in range(nx):
        half, line = x // (nx // 2), x % (nx // 2)

        def spread(c):
            top = c * rows + line * ny
            left = half * nz
            return (
                near[top : top + ny, left : left + nz] + far[top : top + ny, left : left + nz]
            )

        force = [spread(c) for c in range(3)]
        stiff = spread(3)
        result, speed = collide(
            [popul[i, x] for i in range(Q19)], force, solid[x] == 1
        )
        for i in range(Q19):
            post[i, x] = rolled(result[i], i)
        slope[x] = stiff
        for c in range(3):
            field[c, x] = force[c] - stiff * speed[c]
            moved[c, x] = speed[c]

    def value_y(index, at):
        if index < Q19:
            return post[index, :, at, :]
        if index < Q19 + 3:
            return field[index - Q19, :, at, :]
        return solid[:, at, :].astype(f32)

    def value_x(index, at):
        if index < Q19:
            return post[index, at]
        if index < Q19 + 3:
            return field[index - Q19, at]
        return solid[at].astype(f32)

    send_faces(value_y, value_x, 1, 4, nx, ny, *msgs)


def later_kernel(
    nx, ny, nz, post1, field, slope, moved, solid, yd, yu, xd, xu, cd, cu, *refs
):
    post, speeds, y_up, y_down, x_up, x_down, wide, extra, next_wide, speed2 = refs
    wide_rows = 16

    def buffer_of(index):
        if index < Q19:
            return wide, index, 2
        return extra, index - Q19, 1

    for x in range(nx):
        for i in range(Q19):
            wide[i, x + 2, 2 : 2 + ny, :] = post1[i, x]
        for c in range(3):
            extra[c, x + 1, 1 : 1 + ny, :] = field[c, x]
        extra[3, x + 1, 1 : 1 + ny, :] = solid[x].astype(f32)
    fill_halo(buffer_of, 2, 1, 4, nx, ny, (yd, yu), (xd, xu), (cd, cu))

    for x in range(nx + 2):
        popul = []
        for i in range(Q19):
            dx, dy, _ = lattice_dirs[i]
            popul.append(wide[i, x + 1 - dx, 1 - dy : 1 - dy + wide_rows, :])
        force = [extra[c, x, 0:wide_rows, :] for c in range(3)]
        result, speed = collide(popul, force, extra[3, x, 0:wide_rows, :] == 1.0)
        for i in range(Q19):
            next_wide[i, x, 0:wide_rows, :] = rolled(result[i], i)
        for c in range(3):
            speed2[c, x, 0:wide_rows, :] = speed[c]

    rows = (nx // 2) * ny
    for x in range(nx):
        half, line = x // (nx // 2), x % (nx // 2)
        popul = []
        for i in range(Q19):
            dx, dy, _ = lattice_dirs[i]
            popul.append(next_wide[i, x + 1 - dx, 1 - dy : 1 - dy + ny, :])
        before = [speed2[c, x + 1, 1 : 1 + ny, :] for c in range(3)]
        force = [field[c, x] - slope[x] * before[c] for c in range(3)]
        result, speed = collide(popul, force, solid[x] == 1)
        for i in range(Q19):
            post[i, x] = rolled(result[i], i)
        for c in range(3):
            top = c * rows + line * ny
            speeds[top : top + ny, half * nz : (half + 1) * nz] = (
                moved[c, x] + before[c] + speed[c]
            )

    send_faces(
        lambda index, at: post[index, :, at, :],
        lambda index, at: post[index, at],
        0,
        0,
        nx,
        ny,
        y_up,
        y_down,
        x_up,
        x_down,
    )


def last_kernel(nx, ny, post, yd, yu, xd, xu, cd, cu, out, wide):
    for i in range(Q19):
        if lattice_dirs[i][0] == 0 and lattice_dirs[i][1] == 0:
            continue
        for x in range(nx):
            wide[i, x + 1, 1 : 1 + ny, :] = post[i, x]
    fill_halo(lambda index: (wide, index, 1), 1, 0, 0, nx, ny, (yd, yu), (xd, xu), (cd, cu))
    for i in range(Q19):
        dx, dy, _ = lattice_dirs[i]
        for x in range(nx):
            if dx == 0 and dy == 0:
                out[i, x] = post[i, x]
            else:
                out[i, x] = wide[i, x + 1 - dx, 1 - dy : 1 - dy + ny, :]


def exchange(messages, reach, extras, nx, nz):
    y_up, y_down, x_up, x_down = messages
    from_down = shifted(y_up, "yz", 1)
    from_up = shifted(y_down, "yz", -1)
    from_left = shifted(x_up, "gx", 1)
    from_right = shifted(x_down, "gx", -1)
    rows = corner_rows(reach, extras)
    to_up, to_down = call(
        functools.partial(corner_kernel, reach, extras, nx),
        (from_down, from_up),
        [((rows, nz), f32)] * 2,
        name="corner",
    )
    corner_left = shifted(to_up, "gx", 1)
    corner_right = shifted(to_down, "gx", -1)
    return from_down, from_up, from_left, from_right, corner_left, corner_right


def body(populations, solid, displacement, stiffness, marker_tile, marker_site):
    across = lax.axis_size("yz")
    nx, ny, nz = solid.shape
    count = displacement.shape[1]
    padded = round_up(count, 128)
    rows, lanes = (nx // 2) * ny, 2 * nz

    (raw,) = call(
        functools.partial(pack_kernel, nx, ny, nz),
        (
            displacement,
            stiffness.reshape(1, count),
            marker_tile.reshape(1, count),
            marker_site.reshape(1, count),
        ),
        [((8, padded), f32)],
        name="pack",
    )
    near = [raw] + [shifted(raw, "yz", steps) for steps in range(1, across)]
    far = [shifted(value, "gx", 1) for value in near]
    (near_field,) = call(
        functools.partial(scatter_kernel, rows, lanes, False, across),
        near,
        [((4 * rows, lanes), f32)],
        name="scatter_near",
    )
    (far_field,) = call(
        functools.partial(scatter_kernel, rows, lanes, True, across),
        far,
        [((4 * rows, lanes), f32)],
        name="scatter_far",
    )

    faces = [len(halo_entries(1, 1, 1, 4)), len(halo_entries(0, 1, 1, 4))]
    post, field, slope, moved, *messages = call(
        functools.partial(first_kernel, nx, ny, nz),
        (populations, solid, near_field, far_field),
        [
            ((Q19, nx, ny, nz), f32),
            ((3, nx, ny, nz), f32),
            ((nx, ny, nz), f32),
            ((3, nx, ny, nz), f32),
            ((faces[0], nx, nz), f32),
            ((faces[0], nx, nz), f32),
            ((faces[1], ny, nz), f32),
            ((faces[1], ny, nz), f32),
        ],
        name="first",
    )
    halos = exchange(messages, 1, 4, nx, nz)
    faces = [len(halo_entries(1, 1, 0, 0)), len(halo_entries(0, 1, 0, 0))]
    post, speeds, *messages = call(
        functools.partial(later_kernel, nx, ny, nz),
        (post, field, slope, moved, solid) + halos,
        [
            ((Q19, nx, ny, nz), f32),
            ((3 * rows, lanes), f32),
            ((faces[0], nx, nz), f32),
            ((faces[0], nx, nz), f32),
            ((faces[1], ny, nz), f32),
            ((faces[1], ny, nz), f32),
        ],
        scratch=[
            pltpu.VMEM((Q19, nx + 4, 24, nz), f32),
            pltpu.VMEM((4, nx + 2, 16, nz), f32),
            pltpu.VMEM((Q19, nx + 2, 16, nz), f32),
            pltpu.VMEM((3, nx + 2, 16, nz), f32),
        ],
        name="later",
    )
    halos = exchange(messages, 0, 0, nx, nz)
    returns = call(
        functools.partial(gather_kernel, rows, lanes, across),
        [speeds] + near + far,
        [((8, padded), f32)] * across,
        name="gather",
    )
    back = [returns[0]] + [shifted(returns[steps], "yz", -steps) for steps in range(1, across)]
    near_sum, far_sum = call(
        functools.partial(own_sum_kernel, across),
        [displacement] + back,
        [((3, count), f32), ((8, padded), f32)],
        name="own_sum",
    )
    far_back = shifted(far_sum, "gx", -1)
    (final,) = call(
        functools.partial(last_kernel, nx, ny),
        (post,) + halos,
        [((Q19, nx, ny, nz), f32)],
        scratch=[pltpu.VMEM((Q19, nx + 2, 16, nz), f32)],
        name="last",
        hbm_outs=True,
    )
    (final_moved,) = call(
        add_far_kernel,
        (near_sum, far_back),
        [((3, count), f32)],
        name="add_far",
        hbm_outs=True,
    )
    return final, final_moved


def solution(mesh):
    in_specs = (
        P(None, "gx", "yz", None),
        P("gx", "yz", None),
        P(None, ("gx", "yz")),
        P(("gx", "yz")),
        P(("gx", "yz"), None),
        P(("gx", "yz")),
    )
    out_specs = (P(None, "gx", "yz", None), P(None, ("gx", "yz")))
    return jax.shard_map(body, mesh=mesh, in_specs=in_specs, out_specs=out_specs, check_vma=False)
```

```python
import functools

import jax
import jax.numpy as jnp
from jax import lax
from jax.experimental import pallas as pl
from jax.experimental.pallas import tpu as pltpu
from jax.sharding import PartitionSpec as P

STEPS = 3

lattice_dirs = [
    (0, 0, 0),
    (1, 0, 0),
    (-1, 0, 0),
    (0, 1, 0),
    (0, -1, 0),
    (0, 0, 1),
    (0, 0, -1),
    (1, 1, 0),
    (-1, -1, 0),
    (1, -1, 0),
    (-1, 1, 0),
    (1, 0, 1),
    (-1, 0, -1),
    (1, 0, -1),
    (-1, 0, 1),
    (0, 1, 1),
    (0, -1, -1),
    (0, 1, -1),
    (0, -1, 1),
]
lattice_weights = [1.0 / 3.0] + [1.0 / 18.0] * 6 + [1.0 / 36.0] * 12
opposite_dirs = [0, 2, 1, 4, 3, 6, 5, 8, 7, 10, 9, 12, 11, 14, 13, 16, 15, 18, 17]
relax_rate = 1.6
Q19 = len(lattice_dirs)


f32 = jnp.float32
bf16 = jnp.bfloat16


def in_vmem(value):
    return pltpu.with_memory_space_constraint(value, pltpu.VMEM)


def call(kernel, args, outs, scratch=(), name=None, far_args=(), hbm_outs=False):
    if hbm_outs:
        out_shape = [jax.ShapeDtypeStruct(shape, dtype) for shape, dtype in outs]
    else:
        out_shape = [pltpu.VMEM(shape, dtype) for shape, dtype in outs]
    spec = pl.BlockSpec(memory_space=pltpu.VMEM)
    far_spec = pl.BlockSpec(memory_space=pl.ANY)
    return pl.pallas_call(
        kernel,
        out_shape=out_shape,
        in_specs=[far_spec] * len(far_args) + [spec] * len(args),
        out_specs=[spec] * len(outs),
        scratch_shapes=list(scratch),
        name=name,
    )(*far_args, *[in_vmem(arg) for arg in args])


def shifted(value, axis, steps):
    count = lax.axis_size(axis)
    pairs = [(source, (source + steps) % count) for source in range(count)]
    return lax.ppermute(value, axis, pairs)


def total_of(values):
    values = list(values)
    while len(values) > 1:
        paired = [values[i] + values[i + 1] for i in range(0, len(values) - 1, 2)]
        if len(values) % 2:
            paired.append(values[-1])
        values = paired
    return values[0]


def along(offsets, parts):
    total = None
    for component in range(3):
        if offsets[component] == 0:
            continue
        part = parts[component]
        if total is None:
            total = part if offsets[component] > 0 else -part
        else:
            total = total + part if offsets[component] > 0 else total - part
    return total


def collide(popul, field, solid):
    density = total_of(popul)
    inverse = 1.0 / density
    speed = []
    for component in range(3):
        plus = [popul[i] for i in range(Q19) if lattice_dirs[i][component] > 0]
        minus = [popul[i] for i in range(Q19) if lattice_dirs[i][component] < 0]
        total = total_of(plus) - total_of(minus) + 0.5 * field[component]
        speed.append(total * inverse)
    squared = total_of([part * part for part in speed])
    work = total_of([speed[c] * field[c] for c in range(3)])
    keep = 1.0 - relax_rate
    gain = 1.0 - 0.5 * relax_rate
    scaled = relax_rate * density
    base = scaled * (1.0 - 1.5 * squared) - (3.0 * gain) * work
    quad = 4.5 * scaled
    lin = 3.0 * scaled
    result = [None] * Q19
    for index in range(Q19):
        other = opposite_dirs[index]
        weight = lattice_weights[index]
        if index == other:
            post = keep * popul[index] + weight * base
            result[index] = jnp.where(solid, popul[index], post)
            continue
        if other < index:
            continue
        moved = along(lattice_dirs[index], speed)
        pushed = along(lattice_dirs[index], field)
        even = base + moved * (quad * moved + (9.0 * gain) * pushed)
        odd = lin * moved + (3.0 * gain) * pushed
        first = keep * popul[index] + weight * (even + odd)
        second = keep * popul[other] + weight * (even - odd)
        result[index] = jnp.where(solid, popul[other], first)
        result[other] = jnp.where(solid, popul[index], second)
    return result, speed


def rolled(value, index):
    steps = lattice_dirs[index][2]
    if steps == 0:
        return value
    size = value.shape[-1]
    return pltpu.roll(value, steps % size, len(value.shape) - 1)


def halo_entries(axis, sign, reach, extras):
    entries = []
    for layer in range(1, reach + 2):
        for index in range(Q19):
            if sign * lattice_dirs[index][axis] >= layer - reach:
                entries.append((index, layer))
    entries += [(Q19 + extra, 1) for extra in range(extras)]
    return entries


def corner_entries(sign_x, sign_y, reach, extras):
    rows = []
    for place, (index, layer_y) in enumerate(halo_entries(1, sign_y, reach, extras)):
        for layer_x in range(1, reach + 2):
            if index >= Q19:
                if layer_x == 1:
                    rows.append((place, layer_x, index, layer_y))
            elif sign_x * lattice_dirs[index][0] >= layer_x - reach:
                rows.append((place, layer_x, index, layer_y))
    return rows


def face_index(size, sign, layer):
    return size - layer if sign > 0 else layer - 1


def halo_index(size, sign, layer):
    return -layer if sign > 0 else size - 1 + layer


def round_up(count, unit):
    return (count + unit - 1) // unit * unit


def write_corners(reach, extras, nx, sources, targets):
    for sign_x, (target, at) in ((1, targets[0]), (-1, targets[1])):
        for sign_y, source in ((1, sources[0]), (-1, sources[1])):
            for place, layer_x, _, _ in corner_entries(sign_x, sign_y, reach, extras):
                row = place * nx + face_index(nx, sign_x, layer_x)
                target[at : at + 1, :] = source[row : row + 1, :]
                at += 1


def corner_kernel(reach, extras, nx, from_down, from_up, to_up, to_down):
    for target in (to_up, to_down):
        target[...] = jnp.zeros(target.shape, f32)
    write_corners(reach, extras, nx, (from_down, from_up), ((to_up, 0), (to_down, 0)))


def corner_rows(reach, extras):
    return max(sum(len(corner_entries(x, y, reach, extras)) for y in (1, -1)) for x in (1, -1))


def fill_halo(buffer_of, pad, reach, extras, nx, ny, y_msgs, x_msgs, corners):
    for sign, message in ((1, y_msgs[0]), (-1, y_msgs[1])):
        for place, (index, layer) in enumerate(halo_entries(1, sign, reach, extras)):
            ref, at, margin = buffer_of(index)
            row = halo_index(ny, sign, layer) + margin
            ref[at, margin : margin + nx, row, :] = message[place * nx : (place + 1) * nx, :]
    for sign, message in ((1, x_msgs[0]), (-1, x_msgs[1])):
        for place, (index, layer) in enumerate(halo_entries(0, sign, reach, extras)):
            ref, at, margin = buffer_of(index)
            column = halo_index(nx, sign, layer) + margin
            ref[at, column, margin : margin + ny, :] = message[place * ny : (place + 1) * ny, :]
    for sign_x, (message, place) in ((1, corners[0]), (-1, corners[1])):
        for sign_y in (1, -1):
            for _, layer_x, index, layer_y in corner_entries(sign_x, sign_y, reach, extras):
                ref, at, margin = buffer_of(index)
                column = halo_index(nx, sign_x, layer_x) + margin
                row = halo_index(ny, sign_y, layer_y) + margin
                ref[at, column, row : row + 1, :] = message[place : place + 1, :]
                place += 1


def send_faces(value_y, value_x, reach, extras, nx, ny, y_up, y_down, x_up, x_down):
    for sign, message in ((1, y_up), (-1, y_down)):
        for place, (index, layer) in enumerate(halo_entries(1, sign, reach, extras)):
            message[place * nx : (place + 1) * nx, :] = value_y(index, face_index(ny, sign, layer))
    for sign, message in ((1, x_up), (-1, x_down)):
        for place, (index, layer) in enumerate(halo_entries(0, sign, reach, extras)):
            message[place * ny : (place + 1) * ny, :] = value_x(index, face_index(nx, sign, layer))


def pack_kernel(nx, ny, nz, *refs):
    far, out, start, near, sems = refs[:4], refs[4], refs[5], refs[6:10], refs[10]
    copies = [pltpu.make_async_copy(far[i], near[i], sems.at[i]) for i in range(4)]
    for copy in copies:
        copy.start()
    for copy in copies:
        copy.wait()
    moved, stiff, tile, site = near
    count = moved.shape[1]
    half = (nx // 2) * ny * nz
    place = site[...]
    high = place // half
    rest = place - high * half
    row = rest // nz
    lane = rest - row * nz + high * nz
    out[...] = jnp.concatenate(
        [jnp.zeros((6, out.shape[1]), f32), jnp.full((2, out.shape[1]), -1.0, f32)], axis=0
    )
    out[0:3, 0:count] = -stiff[...] * moved[...]
    out[3:4, 0:count] = stiff[...]
    out[4:5, 0:count] = lane.astype(f32)
    out[5:6, 0:count] = row.astype(f32)
    out[6:7, 0:count] = tile[...].astype(f32)
    start[...] = jnp.zeros(start.shape, f32)
    start[0:3, 0:count] = moved[...]


def one_hot(values, size, dtype=bf16):
    places = lax.broadcasted_iota(jnp.int32, (size, values.shape[1]), 0).astype(f32)
    return jnp.where(places == values, 1.0, 0.0).astype(dtype)


def two_parts(value):
    high = value.astype(bf16)
    low = (value - high.astype(f32)).astype(bf16)
    return high, low


def wanted_slot(far):
    slot = lax.axis_index("yz")
    if far:
        slot = slot + lax.axis_size("yz")
    return slot.astype(f32)


def marker_rows(raw, far):
    return jnp.where(raw[6:7, :] == wanted_slot(far), raw[5:6, :], -1.0)


def scatter(rows, lanes, far, raws):
    total = jnp.zeros((8 * rows, lanes), f32)
    for raw in raws:
        high, low = two_parts(raw[0:4, :])
        mask = one_hot(marker_rows(raw, far), rows)
        left = jnp.concatenate(
            [mask * part[c : c + 1, :] for part in (high, low) for c in range(4)], axis=0
        )
        right = one_hot(raw[4:5, :], lanes)
        total = total + lax.dot_general(
            left, right, (((1,), (1,)), ((), ())), preferred_element_type=f32
        )
    return total[: 4 * rows] + total[4 * rows :]


def near_kernel(rows, lanes, count, popul_far, solid_far, *refs):
    raws, out, popul, solid, sems = refs[:count], refs[count], *refs[count + 1 : count + 4]
    copies = [
        pltpu.make_async_copy(popul_far, popul, sems.at[0]),
        pltpu.make_async_copy(solid_far, solid, sems.at[1]),
    ]
    for copy in copies:
        copy.start()
    out[...] = scatter(rows, lanes, False, raws)
    for copy in copies:
        copy.wait()


def far_kernel(rows, lanes, count, *refs):
    refs[count + 1][...] = refs[count][...] + scatter(rows, lanes, True, refs[:count])


def gather_kernel(rows, lanes, halo_rows, speed, near, far, *refs):
    out, kept = refs[-2:]
    high, low = two_parts(speed[...])
    table = jnp.concatenate([high, low], axis=0)
    for kind, raw in enumerate((near, far)):
        right = one_hot(raw[4:5, :], lanes)
        picked = lax.dot_general(
            table, right, (((1,), (0,)), ((), ())), preferred_element_type=f32
        )
        mask = one_hot(marker_rows(raw, kind == 1), rows, f32)
        for c in range(3):
            part = picked[c * rows : (c + 1) * rows] + picked[(3 + c) * rows : (4 + c) * rows]
            kept[3 * kind + c : 3 * kind + c + 1, :] = jnp.sum(part * mask, axis=0, keepdims=True)
    if halo_rows:
        out[0:halo_rows, :] = refs[0][...]
    width = out.shape[1]
    for tile in range(kept.shape[1] // width):
        at = halo_rows + 6 * tile
        out[at : at + 6, :] = kept[0:6, tile * width : (tile + 1) * width]


def turn_kernel(nx, ny, halo_rows, count, start, y_up, y_down, x_up, x_down, *refs):
    parts, (near_sum, to_up, to_down) = refs[:count], refs[count:]
    width = to_up.shape[1]
    face, corner = x_up.shape[0], corner_rows(0, 0)
    for target in (to_up, to_down):
        target[face:, :] = jnp.zeros((target.shape[0] - face, width), f32)
    to_up[0:face, :] = x_up[...]
    to_down[0:face, :] = x_down[...]
    write_corners(0, 0, nx, (y_up, y_down), ((to_up, face), (to_down, face)))
    for tile in range(start.shape[1] // width):
        total = total_of(
            [part[at + 6 * tile : at + 6 * tile + 6, :] for part, at in zip(parts, halo_rows)]
        )
        lanes = slice(tile * width, (tile + 1) * width)
        near_sum[0:3, lanes] = start[0:3, lanes] + total[0:3]
        at = face + corner + 3 * tile
        to_down[at : at + 3, :] = total[3:6]


def first_kernel(nx, ny, nz, popul, solid, force_in, post, field, slope, moved, *msgs):
    rows = (nx // 2) * ny
    for x in range(nx):
        half, line = x // (nx // 2), x % (nx // 2)

        def spread(c):
            top = c * rows + line * ny
            left = half * nz
            return force_in[top : top + ny, left : left + nz]

        force = [spread(c) for c in range(3)]
        stiff = spread(3)
        result, speed = collide(
            [popul[i, x] for i in range(Q19)], force, solid[x] == 1
        )
        for i in range(Q19):
            post[i, x] = rolled(result[i], i)
        slope[x] = stiff
        for c in range(3):
            field[c, x] = force[c] - stiff * speed[c]
            moved[c, x] = speed[c]

    def value_y(index, at):
        if index < Q19:
            return post[index, :, at, :]
        if index < Q19 + 3:
            return field[index - Q19, :, at, :]
        return solid[:, at, :].astype(f32)

    def value_x(index, at):
        if index < Q19:
            return post[index, at]
        if index < Q19 + 3:
            return field[index - Q19, at]
        return solid[at].astype(f32)

    send_faces(value_y, value_x, 1, 4, nx, ny, *msgs)


def later_kernel(
    nx, ny, nz, post1, field, slope, moved, solid, yd, yu, xd, xu, cd, cu, *refs
):
    post, speeds, y_up, y_down, x_up, x_down, wide, extra, next_wide, speed2 = refs
    wide_rows = 16

    def buffer_of(index):
        if index < Q19:
            return wide, index, 2
        return extra, index - Q19, 1

    for x in range(nx):
        for i in range(Q19):
            wide[i, x + 2, 2 : 2 + ny, :] = post1[i, x]
        for c in range(3):
            extra[c, x + 1, 1 : 1 + ny, :] = field[c, x]
        extra[3, x + 1, 1 : 1 + ny, :] = solid[x].astype(f32)
    fill_halo(buffer_of, 2, 1, 4, nx, ny, (yd, yu), (xd, xu), ((cd, 0), (cu, 0)))

    for x in range(nx + 2):
        popul = []
        for i in range(Q19):
            dx, dy, _ = lattice_dirs[i]
            popul.append(wide[i, x + 1 - dx, 1 - dy : 1 - dy + wide_rows, :])
        force = [extra[c, x, 0:wide_rows, :] for c in range(3)]
        result, speed = collide(popul, force, extra[3, x, 0:wide_rows, :] == 1.0)
        for i in range(Q19):
            next_wide[i, x, 0:wide_rows, :] = rolled(result[i], i)
        for c in range(3):
            speed2[c, x, 0:wide_rows, :] = speed[c]

    rows = (nx // 2) * ny
    for x in range(nx):
        half, line = x // (nx // 2), x % (nx // 2)
        popul = []
        for i in range(Q19):
            dx, dy, _ = lattice_dirs[i]
            popul.append(next_wide[i, x + 1 - dx, 1 - dy : 1 - dy + ny, :])
        before = [speed2[c, x + 1, 1 : 1 + ny, :] for c in range(3)]
        force = [field[c, x] - slope[x] * before[c] for c in range(3)]
        result, speed = collide(popul, force, solid[x] == 1)
        for i in range(Q19):
            post[i, x] = rolled(result[i], i)
        for c in range(3):
            top = c * rows + line * ny
            speeds[top : top + ny, half * nz : (half + 1) * nz] = (
                moved[c, x] + before[c] + speed[c]
            )

    send_faces(
        lambda index, at: post[index, :, at, :],
        lambda index, at: post[index, at],
        0,
        0,
        nx,
        ny,
        y_up,
        y_down,
        x_up,
        x_down,
    )


def last_kernel(nx, ny, post, near_sum, yd, yu, xd, xu, out, moved, wide):
    for i in range(Q19):
        if lattice_dirs[i][0] == 0 and lattice_dirs[i][1] == 0:
            continue
        for x in range(nx):
            wide[i, x + 1, 1 : 1 + ny, :] = post[i, x]
    face, corner = len(halo_entries(0, 1, 0, 0)) * ny, corner_rows(0, 0)
    fill_halo(
        lambda index: (wide, index, 1), 1, 0, 0, nx, ny, (yd, yu), (xd, xu), ((xd, face), (xu, face))
    )
    for i in range(Q19):
        dx, dy, _ = lattice_dirs[i]
        for x in range(nx):
            if dx == 0 and dy == 0:
                out[i, x] = post[i, x]
            else:
                out[i, x] = wide[i, x + 1 - dx, 1 - dy : 1 - dy + ny, :]
    width, number = xu.shape[1], moved.shape[1]
    for tile in range(near_sum.shape[1] // width):
        left = tile * width
        size = min(width, number - left)
        at = face + corner + 3 * tile
        moved[0:3, left : left + size] = near_sum[0:3, left : left + size] + xu[at : at + 3, 0:size]


def body(populations, solid, displacement, stiffness, marker_tile, marker_site):
    across = lax.axis_size("yz")
    nx, ny, nz = solid.shape
    count = displacement.shape[1]
    padded = round_up(count, nz)
    rows, lanes = (nx // 2) * ny, 2 * nz

    raw, start = call(
        functools.partial(pack_kernel, nx, ny, nz),
        (),
        [((8, padded), f32)] * 2,
        scratch=[
            pltpu.VMEM((3, count), f32),
            pltpu.VMEM((1, count), f32),
            pltpu.VMEM((1, count), jnp.int32),
            pltpu.VMEM((1, count), jnp.int32),
            pltpu.SemaphoreType.DMA((4,)),
        ],
        far_args=(
            displacement,
            stiffness.reshape(1, count),
            marker_tile.reshape(1, count),
            marker_site.reshape(1, count),
        ),
        name="pack",
    )
    near = [raw] + [shifted(raw, "yz", steps) for steps in range(1, across)]
    far = [shifted(value, "gx", 1) for value in near]
    field, popul, solid = call(
        functools.partial(near_kernel, rows, lanes, across),
        near,
        [
            ((4 * rows, lanes), f32),
            (populations.shape, f32),
            (solid.shape, jnp.int32),
        ],
        scratch=[pltpu.SemaphoreType.DMA((2,))],
        far_args=(populations, solid),
        name="near",
    )
    (field,) = call(
        functools.partial(far_kernel, rows, lanes, across),
        far + [field],
        [((4 * rows, lanes), f32)],
        name="far",
    )

    y_rows, x_rows = (len(halo_entries(1, 1, 1, 4)) * nx, len(halo_entries(0, 1, 1, 4)) * ny)
    post, field, slope, moved, y_up, y_down, x_up, x_down = call(
        functools.partial(first_kernel, nx, ny, nz),
        (popul, solid, field),
        [
            ((Q19, nx, ny, nz), f32),
            ((3, nx, ny, nz), f32),
            ((nx, ny, nz), f32),
            ((3, nx, ny, nz), f32),
            ((y_rows, nz), f32),
            ((y_rows, nz), f32),
            ((x_rows, nz), f32),
            ((x_rows, nz), f32),
        ],
        name="first",
    )
    from_down = shifted(y_up, "yz", 1)
    from_up = shifted(y_down, "yz", -1)
    from_left = shifted(x_up, "gx", 1)
    from_right = shifted(x_down, "gx", -1)
    corner_up, corner_down = call(
        functools.partial(corner_kernel, 1, 4, nx),
        (from_down, from_up),
        [((round_up(corner_rows(1, 4), 8), nz), f32)] * 2,
        name="corner",
    )
    corner_left = shifted(corner_up, "gx", 1)
    corner_right = shifted(corner_down, "gx", -1)

    y_rows, x_rows = (len(halo_entries(1, 1, 0, 0)) * nx, len(halo_entries(0, 1, 0, 0)) * ny)
    post, speeds, y_up, y_down, x_up, x_down = call(
        functools.partial(later_kernel, nx, ny, nz),
        (
            post,
            field,
            slope,
            moved,
            solid,
            from_down,
            from_up,
            from_left,
            from_right,
            corner_left,
            corner_right,
        ),
        [
            ((Q19, nx, ny, nz), f32),
            ((3 * rows, lanes), f32),
            ((y_rows, nz), f32),
            ((y_rows, nz), f32),
            ((x_rows, nz), f32),
            ((x_rows, nz), f32),
        ],
        scratch=[
            pltpu.VMEM((Q19, nx + 4, 24, nz), f32),
            pltpu.VMEM((4, nx + 2, 16, nz), f32),
            pltpu.VMEM((Q19, nx + 2, 16, nz), f32),
            pltpu.VMEM((3, nx + 2, 16, nz), f32),
        ],
        name="later",
    )

    tile_rows = 6 * (padded // nz)

    def gathered(source, halo):
        halo_rows = 0 if halo is None else y_rows
        (message,) = call(
            functools.partial(gather_kernel, rows, lanes, halo_rows),
            [speeds, near[source], far[source]] + ([] if halo is None else [halo]),
            [((round_up(halo_rows + tile_rows, 8), nz), f32)],
            scratch=[pltpu.VMEM((8, padded), f32)],
            name="gather",
        )
        return message

    parts, offsets = [], []
    for source in range(1, across):
        halo = None
        if source == 1:
            halo = y_down
        elif source == across - 1:
            halo = y_up
        parts.append(shifted(gathered(source, halo), "yz", -source))
        offsets.append(0 if halo is None else y_rows)
    from_up = parts[0]
    from_down = parts[-1] if across > 2 else shifted(y_up, "yz", 1)
    parts.append(gathered(0, None))
    offsets.append(0)
    near_sum, to_up, to_down = call(
        functools.partial(turn_kernel, nx, ny, offsets, across),
        [start, from_down, from_up, x_up, x_down] + parts,
        [
            ((8, padded), f32),
            ((round_up(x_rows + corner_rows(0, 0), 8), nz), f32),
            ((round_up(x_rows + corner_rows(0, 0) + tile_rows // 2, 8), nz), f32),
        ],
        name="turn",
    )
    from_left = shifted(to_up, "gx", 1)
    from_right = shifted(to_down, "gx", -1)
    return call(
        functools.partial(last_kernel, nx, ny),
        (post, near_sum, from_down, from_up, from_left, from_right),
        [((Q19, nx, ny, nz), f32), ((3, count), f32)],
        scratch=[pltpu.VMEM((Q19, nx + 2, 16, nz), f32)],
        name="last",
        hbm_outs=True,
    )


def solution(mesh):
    in_specs = (
        P(None, "gx", "yz", None),
        P("gx", "yz", None),
        P(None, ("gx", "yz")),
        P(("gx", "yz")),
        P(("gx", "yz"), None),
        P(("gx", "yz")),
    )
    out_specs = (P(None, "gx", "yz", None), P(None, ("gx", "yz")))
    return jax.shard_map(body, mesh=mesh, in_specs=in_specs, out_specs=out_specs, check_vma=False)
```
